32 devices in a mesh: rep: 4 (over y, core), row: 4 (over z), col: 2 (over x).
Axes of the slice: x: 2, y: 2, z: 4, core: 2. Of those that a mesh axis runs over, the one named last changes fastest.
Arguments:
- patches: bfloat16 [4096, 588], P(('rep', 'col')), may hold values from -20 to 20
- embed_weight: bfloat16 [588, 6144], P(None, 'row'), may hold values from -1 to 1
- embed_bias: float32 [6144], P('row'), may hold values from -3 to 3
- old_in: bfloat16 [64, 768, 1536], P(('row', 'col')), may hold values from -0.078125 to 0.078125
- old_out: bfloat16 [64, 1536, 768], P(('row', 'col')), may hold values from -0.0546875 to 0.0546875
- restore_id: int32 [1], replicated, may hold values from 0 to 47
- norm_gains: float32 [48, 6144], P(None, 'row'), may hold values from 0.1 to 1.9
- in_biases: float32 [48, 12288], P(None, 'col'), may hold values from -3 to 3
- out_biases: float32 [48, 6144], P(None, 'row'), may hold values from -3 to 3
- final_gain: float32 [6144], P('row'), may hold values from 0.1 to 1.9
- check_weight: bfloat16 [6144, 128], P('row'), may hold values from -0.078125 to 0.078125
Outputs:
- in_weight: bfloat16 [6144, 12288], P('row', 'col')
- out_weight: bfloat16 [12288, 6144], P('col', 'row')
- check_logits: float32 [4096, 128], P(('rep', 'col'))
The draws below stay inside these ranges and needn't reach their ends.
All inputs are finite; a program needn't handle non-finite values.
Results may differ from the reference program's by a relative error of at most 0.0062.
Values may be sent and summed in bfloat16 or wider, within the bound.
No kernel may reach another device: no remote copies, remote signals or barrier semaphores. Data moves between devices by JAX's collectives and lax.ppermute only.
A program may use at most 192 MiB of HBM per device.

```python
import math
import jax
import jax.numpy as jnp
from jax import lax

D = 6144
PATCH = 588
LAYERS_ALL = 48
FF = 12288
OLD_GRID = 8
CHECK = 128
TOKENS = 4096


def draw_patches(key, part):
    base_key, scale_key = jax.random.split(key, 2)
    row_scale = jnp.exp(jax.random.uniform(scale_key, (TOKENS, 1), jnp.float32, math.log(0.5), math.log(5.0)))
    noise_part = jax.random.truncated_normal(base_key, -4.0, 4.0, (TOKENS, PATCH), jnp.float32)
    values = row_scale * noise_part
    return values.astype(jnp.bfloat16)


def draw_embed_weight(key, part):
    entry_key, column_key = jax.random.split(key, 2)
    position = jnp.arange(D, dtype=jnp.float32) / D
    trend_part = math.log(3.0) * (position - 0.5)
    jitter = jax.random.uniform(column_key, (D,), jnp.float32, -1.15, 1.15)
    entries = jax.random.truncated_normal(entry_key, -4.0, 4.0, (PATCH, D), jnp.float32)
    column_scale = jnp.exp(trend_part + jitter)
    return (entries * column_scale[None, :] / math.sqrt(PATCH)).astype(jnp.bfloat16)


def block_levels(key, extent, cuts, smallest, largest):
    factor_of, own = 1.0, jax.random.fold_in(key, 6)
    for dim, parts in cuts:
        draws = jnp.exp(jax.random.uniform(jax.random.fold_in(own, dim), (parts,), jnp.float32, smallest / len(cuts), largest / len(cuts)))
        factor_of = factor_of * jnp.repeat(draws, extent[dim] // parts).reshape([-1 if axis == dim else 1 for axis in range(len(extent))])
    return factor_of


def normal_values(rng, extent, deviation, reach, cuts=(), held_as=jnp.bfloat16):
    values = jax.random.normal(rng, extent, jnp.float32) * deviation
    if len(cuts) > 0:
        values = block_levels(rng, extent, cuts, -0.22, 0.18) * values
    return jnp.clip(values, min=-reach, max=reach).astype(held_as)


def setup_inputs(seed: int = 0) -> dict:
    key_of = jax.random.split(jax.random.key(seed), 12)
    return {
        "patches": draw_patches(jax.random.fold_in(key_of[11], 71), 0),
        "embed_weight": draw_embed_weight(jax.random.fold_in(key_of[11], 71), 0),
        "embed_bias": normal_values(key_of[2], (D,), 0.5, 3.0, ((0, 4),), jnp.float32),
        "old_in": normal_values(key_of[3], (OLD_GRID * OLD_GRID, D // OLD_GRID, FF // OLD_GRID), D ** -0.5, 0.078125, ((0, 8),)),
        "old_out": normal_values(key_of[4], (OLD_GRID * OLD_GRID, FF // OLD_GRID, D // OLD_GRID), FF ** -0.5, 0.0546875, ((0, 8),)),
        "restore_id": jax.random.randint(key_of[5], (1,), 0, LAYERS_ALL).astype(jnp.int32),
        "norm_gains": jnp.clip(1.0 + 0.18 * jax.random.normal(key_of[6], (LAYERS_ALL, D), jnp.float32), 0.1, 1.9),
        "in_biases": normal_values(key_of[7], (LAYERS_ALL, FF), 0.5, 3.0, ((1, 2),), jnp.float32),
        "out_biases": normal_values(key_of[8], (LAYERS_ALL, D), 0.5, 3.0, ((1, 4),), jnp.float32),
        "final_gain": jnp.clip(1.0 + 0.18 * jax.random.normal(key_of[9], (D,), jnp.float32), 0.1, 1.9),
        "check_weight": normal_values(key_of[10], (D, CHECK), D ** -0.5, 0.078125, ((0, 4),)),
    }


EPSILON = 1e-06

def assemble_in(old_tiles):
    tile_grid = old_tiles.reshape(OLD_GRID, OLD_GRID, D // OLD_GRID, FF // OLD_GRID)
    return tile_grid.transpose(0, 2, 1, 3).reshape(D, FF)

def assemble_out(old_tiles):
    tile_grid = old_tiles.reshape(OLD_GRID, OLD_GRID, FF // OLD_GRID, D // OLD_GRID)
    return tile_grid.transpose(1, 2, 0, 3).reshape(FF, D)

def pick_rows(restore_id, param_table):
    selector = (jnp.arange(param_table.shape[0], dtype=jnp.int32)[None, :] == restore_id[:, None]).astype(jnp.float32)
    return jnp.dot(selector, param_table, precision=lax.Precision.HIGHEST)[0]

def norm_rows(values, gain_row):
    feature_count = values.shape[1]
    average = lax.optimization_barrier(jnp.sum(values, axis=1, keepdims=True)) / feature_count
    square_mean = lax.optimization_barrier(jnp.sum(values * values, axis=1, keepdims=True)) / feature_count
    inverse_scale = lax.rsqrt(square_mean - average * average + EPSILON)
    return ((values - average) * inverse_scale * gain_row).astype(jnp.bfloat16)

def reference(patches, embed_weight, embed_bias, old_in, old_out, restore_id, norm_gains, in_biases, out_biases, final_gain, check_weight):
    in_weight = assemble_in(old_in)
    out_weight = assemble_out(old_out)
    layer_gain = pick_rows(restore_id, norm_gains)
    layer_in_bias = pick_rows(restore_id, in_biases)
    layer_out_bias = pick_rows(restore_id, out_biases)
    embedded = jnp.dot(patches, embed_weight, preferred_element_type=jnp.float32) + embed_bias
    normed = norm_rows(embedded, layer_gain)
    pre = jnp.dot(normed, in_weight, preferred_element_type=jnp.float32) + layer_in_bias
    hidden = jax.nn.gelu(pre, approximate=False).astype(jnp.bfloat16)
    updated = embedded + jnp.dot(hidden, out_weight, preferred_element_type=jnp.float32) + layer_out_bias
    final_normed = norm_rows(updated, final_gain)
    check_logits = jnp.dot(final_normed, check_weight, preferred_element_type=jnp.float32)
    return (in_weight, out_weight, check_logits)
```

```python
import functools

import jax
import jax.numpy as jnp
from jax import lax
from jax.experimental import pallas as pl
from jax.experimental.pallas import tpu as pltpu
from jax.sharding import PartitionSpec as P


EPSILON = 1e-06


def swap(value, axis, mask):
    pairs = [(source, source ^ mask) for source in range(lax.axis_size(axis))]
    return lax.ppermute(value, axis, pairs)


def masks(axis):
    return [2**bit for bit in range(lax.axis_size(axis).bit_length() - 1)]


def all_sum(value, axis):
    for mask in masks(axis):
        value = value + swap(value, axis, mask)
    return value


def gather_xor(value, axis):
    for mask in masks(axis):
        value = jnp.concatenate([value, swap(value, axis, mask)], axis=0)
    return value


def scatter_xor(value, axis):
    for mask in reversed(masks(axis)):
        half = value.shape[0] // 2
        value = value[:half] + swap(value[half:].astype(jnp.bfloat16), axis, mask).astype(jnp.float32)
    return value


def row_of(table, restore_id):
    return lax.dynamic_index_in_dim(table, restore_id[0], 0, keepdims=False)


def through(moves, buffers, arrive, leave):
    reads, writes = [], []
    for n, ((source, target), buffer) in enumerate(zip(moves, buffers)):
        reads.append(pltpu.make_async_copy(source, buffer, arrive.at[n]))
        writes.append(pltpu.make_async_copy(buffer, target, leave.at[n]))
    for read in reads:
        read.start()
    for read, write in zip(reads, writes):
        read.wait()
        write.start()
    for write in writes:
        write.wait()


def copy_cost(size):
    return pl.CostEstimate(flops=300 * size, transcendentals=0, bytes_accessed=2 * size)


def block_at(ref, row, row_size, column, column_size):
    return ref.at[pl.ds(pl.multiple_of(row, row_size), row_size), pl.ds(pl.multiple_of(column, column_size), column_size)]


def keep_body(place_ref, old_in, old_out, in_ref, out_ref, in_buffer, out_buffer, arrive, leave, *, kept):
    col = place_ref[2]
    _, tile_rows, tile_cols = old_in.shape
    moves, buffers = [], []
    for j in range(kept):
        target = block_at(in_ref, col * tile_rows, tile_rows, j * tile_cols, tile_cols)
        moves.append((old_in.at[col * kept + j], target))
        buffers.append(in_buffer.at[j])
    for j in range(kept):
        target = block_at(out_ref, j * tile_cols, tile_cols, col * tile_rows, tile_rows)
        moves.append((old_out.at[col * kept + j], target))
        buffers.append(out_buffer.at[j])
    through(moves, buffers, arrive, leave)


def keep_tiles(place, old_in, old_out):
    count, tile_rows, tile_cols = old_in.shape
    kept = count // 2
    hbm = pl.BlockSpec(memory_space=pl.ANY)
    kind = old_in.dtype
    return pl.pallas_call(
        functools.partial(keep_body, kept=kept),
        in_specs=[pl.BlockSpec(memory_space=pltpu.SMEM), hbm, hbm],
        out_specs=[hbm] * 2,
        out_shape=[
            jax.ShapeDtypeStruct((2 * tile_rows, kept * tile_cols), kind),
            jax.ShapeDtypeStruct((kept * tile_cols, 2 * tile_rows), kind),
        ],
        scratch_shapes=[
            pltpu.VMEM((kept, tile_rows, tile_cols), kind),
            pltpu.VMEM((kept, tile_cols, tile_rows), kind),
            pltpu.SemaphoreType.DMA((2 * kept,)),
            pltpu.SemaphoreType.DMA((2 * kept,)),
        ],
        cost_estimate=copy_cost(4 * kept * tile_rows * tile_cols),
        name="keep_tiles",
    )(place, old_in, old_out)


def fill_in_body(place_ref, *refs, parts, counts, rows):
    weight, (buffer, arrive, leave) = refs[-4], refs[-3:]
    rep, row, col = (place_ref[n] for n in range(3))
    moves, buffers, n = [], [], 0
    for k in range(parts):
        first = 0
        for m, count in enumerate(counts):
            part = refs[m * parts + k]
            _, tile_rows, width = part.shape
            for i in range(count):
                column = ((rep ^ k) * rows + (row ^ (first + i))) * width
                target = block_at(weight, (1 - col) * tile_rows, tile_rows, column, width)
                moves.append((part.at[i], target))
                buffers.append(buffer.at[n])
                n += 1
            first += count
    through(moves, buffers, arrive, leave)


def fill(place, parts, weight, body, pieces):
    hbm = pl.BlockSpec(memory_space=pl.ANY)
    return pl.pallas_call(
        body,
        in_specs=[pl.BlockSpec(memory_space=pltpu.SMEM)] + [hbm] * (len(parts) + 1),
        out_specs=hbm,
        out_shape=jax.ShapeDtypeStruct(weight.shape, weight.dtype),
        scratch_shapes=[
            pltpu.VMEM((pieces,) + parts[0].shape[1:], weight.dtype),
            pltpu.SemaphoreType.DMA((pieces,)),
            pltpu.SemaphoreType.DMA((pieces,)),
        ],
        input_output_aliases={1 + len(parts): 0},
        cost_estimate=copy_cost(2 * sum(part.size for part in parts)),
    )(place, *parts, weight)


def cut_body(place_ref, tile_ref, *out_refs):
    row, width = place_ref[1], out_refs[0].shape[-1]
    n = 0
    for ref in out_refs:
        for i in range(ref.shape[0]):
            start = pl.multiple_of((row ^ n) * width, width)
            ref[i] = tile_ref[0, :, pl.ds(start, width)]
            n += 1


def cut_tile(tiles, which, row, counts):
    _, tile_rows, tile_cols = tiles.shape
    width = tile_cols // sum(counts)
    spec = pltpu.PrefetchScalarGridSpec(
        num_scalar_prefetch=1,
        grid=(1,),
        in_specs=[pl.BlockSpec((1, tile_rows, tile_cols), lambda i, s: (s[0], 0, 0))],
        out_specs=[pl.BlockSpec((count, tile_rows, width), lambda i, s: (0, 0, 0)) for count in counts],
    )
    return pl.pallas_call(
        cut_body,
        grid_spec=spec,
        out_shape=[jax.ShapeDtypeStruct((count, tile_rows, width), tiles.dtype) for count in counts],
        name="cut_tile",
    )(jnp.stack([which, row]).astype(jnp.int32), tiles)


def spread(part, axis):
    parts = {0: part}
    for mask in reversed(masks(axis)):
        for k in sorted(parts):
            parts[k ^ mask] = swap(parts[k], axis, mask)
    return [parts[k] for k in sorted(parts)]


def layer_body(place_ref, tokens_ref, scale_ref, bias_ref, tile_ref, *refs, groups, adds):
    pieces = [ref.at[i] for ref in refs[:groups] for i in range(ref.shape[0])]
    sum_ref, hidden_ref = refs[-2:]
    row, width = place_ref[1], pieces[0].shape[-1]
    tokens = tokens_ref[...]
    total = refs[groups][...] if adds else None
    for j, piece in enumerate(pieces):
        start = pl.multiple_of((row ^ j) * width, width)
        pre = jnp.dot(tokens, piece[...], preferred_element_type=jnp.float32)
        pre = pre * scale_ref[...] + bias_ref[row ^ j]
        half = 0.5 * pre
        hidden = (half + half * lax.erf(pre * (0.5**0.5))).astype(jnp.bfloat16)
        hidden_ref[:, pl.ds(start, width)] = hidden
        term = jnp.dot(hidden, tile_ref[0, pl.ds(start, width), :], preferred_element_type=jnp.float32)
        total = term if total is None else total + term
    sum_ref[...] = total


def came_body(place_ref, *refs, first, shares, halves, fills):
    value_refs, part_refs = refs[:shares], refs[shares : shares * (1 + halves)]
    refs = refs[shares * (1 + halves) + fills :]
    sum_ref, refs = refs[0], refs[1:]
    weight, refs = (refs[0], refs[1:]) if fills else (None, refs)
    values, parts, arrive, leave, total = refs
    rep, col = place_ref[0], place_ref[2]
    count, width = values.shape[1:]
    height, features = parts.shape[1] // halves, parts.shape[2]
    reads = []
    for k in range(shares):
        group = [pltpu.make_async_copy(value_refs[k].at[pl.ds(first, count)], values.at[k], arrive.at[k, 0])]
        for h in range(halves):
            group.append(
                pltpu.make_async_copy(
                    part_refs[k * halves + h].at[0], parts.at[k, pl.ds(h * height, height)], arrive.at[k, 1 + h]
                )
            )
        for copy in group:
            copy.start()
        reads.append(group)
    writes = []
    for k in range(shares):
        for copy in reads[k]:
            copy.wait()
        if fills:
            target = block_at(weight, (rep ^ k) * width, width, (1 - col) * features, features)
            writes.append(pltpu.make_async_copy(parts.at[k], target, leave.at[k]))
            writes[-1].start()
        term = jnp.dot(values[k], parts[k], preferred_element_type=jnp.float32)
        if k == 0:
            total[...] = term
        elif k < shares - 1:
            total[...] += term
        else:
            sum_ref[...] = (total[...] + term).astype(sum_ref.dtype)
    for copy in writes:
        copy.wait()


def came_sum(place, values, parts, first, count, kind, weight):
    shares, halves = len(values), len(parts) // len(values)
    width, features = values[0].shape[1], parts[0].shape[2]
    hbm = pl.BlockSpec(memory_space=pl.ANY)
    fills = weight is not None
    outs = [jax.ShapeDtypeStruct((count, features), kind)]
    return pl.pallas_call(
        functools.partial(came_body, first=first, shares=shares, halves=halves, fills=int(fills)),
        in_specs=[pl.BlockSpec(memory_space=pltpu.SMEM)] + [hbm] * (len(values) + len(parts) + fills),
        out_specs=[pl.BlockSpec(memory_space=pltpu.VMEM)] + [hbm] * fills,
        out_shape=outs + ([jax.ShapeDtypeStruct(weight.shape, weight.dtype)] if fills else []),
        scratch_shapes=[
            pltpu.VMEM((shares, count, width), values[0].dtype),
            pltpu.VMEM((shares, width, features), parts[0].dtype),
            pltpu.SemaphoreType.DMA((shares, 1 + halves)),
            pltpu.SemaphoreType.DMA((shares,)),
            pltpu.VMEM((count, features), jnp.float32),
        ],
        input_output_aliases={1 + len(values) + len(parts): 1} if fills else {},
        cost_estimate=pl.CostEstimate(
            flops=2 * count * shares * width * features,
            transcendentals=0,
            bytes_accessed=2 * shares * width * (count + features),
        ),
        name="came_sum",
    )(place, *values, *parts, *((weight,) if fills else ()))


def layer_share(place, tokens, scale, bias, tiles, pieces, total, block):
    count, depth = tokens.shape
    _, tile_rows, tile_cols = tiles.shape
    spec = pltpu.PrefetchScalarGridSpec(
        num_scalar_prefetch=1,
        grid=(count // block,),
        in_specs=[
            pl.BlockSpec((block, depth), lambda i, s: (i, 0)),
            pl.BlockSpec((block, 1), lambda i, s: (i, 0)),
            pl.BlockSpec(bias.shape, lambda i, s: (0, 0, 0)),
            pl.BlockSpec((1, tile_rows, tile_cols), lambda i, s: (s[0], 0, 0)),
        ]
        + [pl.BlockSpec(piece.shape, lambda i, s: (0, 0, 0)) for piece in pieces]
        + ([] if total is None else [pl.BlockSpec((block, tile_cols), lambda i, s: (i, 0))]),
        out_specs=[
            pl.BlockSpec((block, tile_cols), lambda i, s: (i, 0)),
            pl.BlockSpec((block, tile_rows), lambda i, s: (i, 0)),
        ],
    )
    return pl.pallas_call(
        functools.partial(layer_body, groups=len(pieces), adds=total is not None),
        grid_spec=spec,
        out_shape=[
            jax.ShapeDtypeStruct((count, tile_cols), jnp.float32),
            jax.ShapeDtypeStruct((count, tile_rows), jnp.bfloat16),
        ],
        input_output_aliases={} if total is None else {5 + len(pieces): 0},
        cost_estimate=pl.CostEstimate(
            flops=2 * count * tile_rows * (depth + tile_cols),
            transcendentals=count * tile_rows,
            bytes_accessed=2 * tile_rows * (tile_cols + depth) + count * (8 * tile_cols + 2 * tile_rows),
        ),
        name="layer_share",
    )(place, tokens, scale, bias, tiles, *pieces, *(() if total is None else (total,)))


def move_halves(pieces, axis):
    index = lax.axis_index(axis)
    for bit, mask in enumerate(masks(axis)):
        upper_side = index >> bit & 1 == 1
        outgoing = tuple(jnp.where(upper_side, low, high) for low, high in pieces)
        incoming = tuple(swap(part, axis, mask) for part in outgoing)
        pieces = tuple(
            (jnp.where(upper_side, came, low), jnp.where(upper_side, high, came))
            for (low, high), came in zip(pieces, incoming)
        )
    return pieces


def relayout_any(old_in, old_out):
    tiles_here, tile_rows, tile_cols = old_in.shape
    local_cols = tiles_here * tile_cols
    half = local_cols // 2
    in_local = jnp.transpose(old_in, (1, 0, 2)).reshape(tile_rows, local_cols)
    out_local = old_out.reshape(local_cols, tile_rows)
    in_pair, out_pair = move_halves(
        ((in_local[:, :half], in_local[:, half:]), (out_local[:half], out_local[half:])), "col"
    )
    return jnp.concatenate(in_pair, axis=0), jnp.concatenate(out_pair, axis=1)


def on_device(
    patches,
    embed_weight,
    embed_bias,
    old_in,
    old_out,
    restore_id,
    norm_gains,
    in_biases,
    out_biases,
    final_gain,
    check_weight,
):
    reps, rows, cols = (lax.axis_size(axis) for axis in ("rep", "row", "col"))
    rep, row, col = (lax.axis_index(axis) for axis in ("rep", "row", "col"))
    tiles_here, tile_rows, tile_cols = old_in.shape
    tokens, patch = patches.shape
    features = embed_weight.shape[1]
    feature_count = features * rows
    depth = -(-(patch + 1) // 16) * 16
    pair = cols == 2 and reps == 4 and tiles_here == 2 * reps and features == 2 * tile_rows and tile_cols % (128 * rows) == 0

    if pair:
        kept = tiles_here // 2
        own, away = col * kept, (1 - col) * kept
        cut = [rows // 2, rows - rows // 2]
        in_sent = cut_tile(old_in, away + rep, row, cut)
        in_sent, embed_weight, embed_bias, patches = lax.optimization_barrier(
            (in_sent, embed_weight, embed_bias, patches)
        )
        in_came = [None] * len(cut)
        for m in reversed(range(len(cut))):
            in_came[m] = swap(in_sent[m], "col", 1)
        in_mine = cut_tile(old_in, own + rep, row, cut)
        where = jnp.stack([rep, row, col]).astype(jnp.int32)
        in_weight, out_weight = keep_tiles(where, old_in, old_out)
    else:
        in_weight, out_weight = relayout_any(old_in, old_out)

    def mine_first(values, axis):
        return jnp.roll(values, -col * tile_rows, axis) if pair else values

    layer_gain = mine_first(row_of(norm_gains, restore_id), 0)
    in_bias = row_of(in_biases, restore_id)
    out_bias = mine_first(row_of(out_biases, restore_id), 0)
    embed_weight = mine_first(embed_weight, 1)
    embed_bias = mine_first(embed_bias, 0)
    final_gain = mine_first(final_gain, 0)
    check_weight = mine_first(check_weight, 0)

    embedded = jnp.dot(patches, embed_weight, preferred_element_type=jnp.float32) + embed_bias
    weight_f32 = embed_weight.astype(jnp.float32)
    sums = all_sum(
        jnp.concatenate(
            [
                jnp.sum(embedded, axis=1),
                jnp.sum(embedded * embedded, axis=1),
                jnp.sum(weight_f32, axis=1),
                jnp.sum(embed_bias)[None],
            ]
        ),
        "row",
    ) / feature_count
    one, late, sums = lax.optimization_barrier((jnp.ones((tokens, 1), patches.dtype), (1 - col) * (tiles_here // 2), sums))
    tokens_in = jnp.concatenate(
        [patches, one, jnp.zeros((tokens, depth - patch - 1), patches.dtype)], axis=1
    )
    tokens_in = gather_xor(tokens_in, "col")
    if pair:
        height = tile_cols // 2

        def out_half(k, half):
            sent = lax.dynamic_slice(old_out, (late + (rep ^ k), half * height, 0), (1, height, tile_rows))
            return swap(sent, "col", 1)

        out_parts = {(0, 0): out_half(0, 0), (0, 1): out_half(0, 1), (2, 1): out_half(2, 1)}

    average, square = sums[:tokens], sums[tokens : 2 * tokens]
    scale = gather_xor(lax.rsqrt(square - average * average + EPSILON), "col")[:, None]

    centers = sums[2 * tokens :]
    centered = jnp.concatenate(
        [
            (weight_f32 - centers[:patch, None]) * layer_gain,
            ((embed_bias - centers[patch]) * layer_gain)[None],
            jnp.zeros((depth - patch - 1, features), jnp.float32),
        ]
    ).astype(jnp.bfloat16)
    hidden_here = in_weight.shape[1]
    share = hidden_here // reps
    piece = share // rows

    def times(left, right):
        return jnp.dot(left, right, preferred_element_type=jnp.float32)

    def partial(k):
        if not pair:
            return times(centered, lax.dynamic_slice_in_dim(in_weight, rep * share + (row ^ k) * piece, piece, 1))
        m, i = (0, k) if k < cut[0] else (1, k - cut[0])
        return times(centered[:, :tile_rows], in_mine[m][i]) + times(centered[:, tile_rows:], in_came[m][i])

    came = [swap(partial(k).astype(jnp.bfloat16), "row", k) for k in reversed(range(1, rows))]
    folded = partial(0)
    for value in came:
        folded = folded + value.astype(jnp.float32)
    folded = folded.astype(jnp.bfloat16)
    group = spread(folded, "row")

    if pair:
        groups = {0: group}
        for mask in reversed(masks("rep")):
            for k in sorted(groups):
                if mask > 1:
                    groups[k ^ mask] = [swap(value, "rep", mask) for value in groups[k]]
                else:
                    groups[k ^ mask] = [swap(jnp.stack(groups[k]), "rep", mask)]
        in_parts = [spread(part, "rep") for part in in_came]
        out_parts[2, 0] = swap(out_parts[0, 0], "rep", 2)
        for k, half in sorted(out_parts):
            out_parts[k ^ 1, half] = swap(out_parts[k, half], "rep", 1)
        in_weight = fill(
            where,
            [part for parts in in_parts for part in parts],
            in_weight,
            functools.partial(fill_in_body, parts=reps, counts=cut, rows=rows),
            reps * rows,
        )
        biases = in_bias.reshape(reps, rows, 1, piece)
        branch_mine = None
        order = sorted(groups, key=lambda k: (bin(k).count("1"), k))
        values = {}
        for k in order:
            pieces = [value if value.ndim == 3 else value[None] for value in groups[k]]
            place = jnp.stack([own + (rep ^ k), row]).astype(jnp.int32)
            bias = lax.dynamic_index_in_dim(biases, rep ^ k, 0, keepdims=False)
            branch_mine, values[k] = layer_share(
                place, tokens_in, scale, bias, old_out, pieces, branch_mine, min(256, tokens_in.shape[0])
            )

        shares = [values[k] for k in sorted(values)]
        parts = [out_parts[key] for key in sorted(out_parts)]
        to_came = swap(branch_mine[tokens:].astype(jnp.bfloat16), "col", 1).astype(jnp.float32)
        theirs, out_weight = came_sum(where, shares, parts, tokens, tokens, jnp.bfloat16, out_weight)
        to_mine = swap(theirs, "col", 1).astype(jnp.float32)
        (branch_came,) = came_sum(where, shares, parts, 0, tokens, jnp.float32, None)
        branch = jnp.concatenate([branch_mine[:tokens] + to_mine, branch_came + to_came], axis=1)
    else:
        group = jnp.take(jnp.stack(group), row ^ jnp.arange(rows), axis=0)
        shares = jnp.take(jnp.stack(spread(group, "rep")), rep ^ jnp.arange(reps), axis=0)
        folded = jnp.transpose(shares, (2, 0, 1, 3)).reshape(depth, hidden_here)
        pre = times(tokens_in, folded) * scale + in_bias
        hidden = (0.5 * pre * (1.0 + lax.erf(pre * (0.5**0.5)))).astype(jnp.bfloat16)
        branch = scatter_xor(times(hidden, out_weight), "col")
    updated = embedded + branch + out_bias

    center = jnp.mean(updated, axis=1, keepdims=True)
    weighted = final_gain[:, None] * check_weight.astype(jnp.float32)
    slope = jnp.sum(weighted, axis=0, keepdims=True)
    logits = times(((updated - center) * final_gain).astype(jnp.bfloat16), check_weight) + center * slope
    checks = logits.shape[1]
    moments = jnp.concatenate([jnp.sum(updated, axis=1), jnp.sum(updated * updated, axis=1), slope[0]])
    moments = jnp.pad(moments, (0, -moments.size % (8 * checks))).reshape(-1, checks)
    total = all_sum(jnp.concatenate([logits, moments]), "row")
    moments = total[tokens:].reshape(-1)
    average = moments[:tokens, None] / feature_count
    variance = moments[tokens : 2 * tokens, None] / feature_count - average * average
    slope = moments[None, 2 * tokens : 2 * tokens + checks]
    check_logits = (total[:tokens] - average * slope) * lax.rsqrt(variance + EPSILON)
    return (in_weight, out_weight, check_logits)


def solution(mesh):
    placed = (
        P(("rep", "col"), None),
        P(None, "row"),
        P("row"),
        P(("row", "col"), None, None),
        P(("row", "col"), None, None),
        P(),
        P(None, "row"),
        P(None, "col"),
        P(None, "row"),
        P("row"),
        P("row", None),
    )
    return jax.shard_map(
        on_device,
        mesh=mesh,
        in_specs=placed,
        out_specs=(P("row", "col"), P("col", "row"), P(("rep", "col"), None)),
        check_vma=False,
    )
```

```python
import functools

import jax
import jax.numpy as jnp
from jax import lax
from jax.experimental import pallas as pl
from jax.experimental.pallas import tpu as pltpu
from jax.sharding import PartitionSpec as P


EPSILON = 1e-06


def swap(value, axis, mask):
    pairs = [(source, source ^ mask) for source in range(lax.axis_size(axis))]
    return lax.ppermute(value, axis, pairs)


def masks(axis):
    return [2**bit for bit in range(lax.axis_size(axis).bit_length() - 1)]


def all_sum(value, axis):
    for mask in masks(axis):
        value = value + swap(value, axis, mask)
    return value


def gather_xor(value, axis):
    for mask in masks(axis):
        value = jnp.concatenate([value, swap(value, axis, mask)], axis=0)
    return value


def scatter_xor(value, axis):
    for mask in reversed(masks(axis)):
        half = value.shape[0] // 2
        value = value[:half] + swap(value[half:].astype(jnp.bfloat16), axis, mask).astype(jnp.float32)
    return value


def row_of(table, restore_id):
    return lax.dynamic_index_in_dim(table, restore_id[0], 0, keepdims=False)


def through(moves, buffers, arrive, leave):
    reads, writes = [], []
    for n, ((source, target), buffer) in enumerate(zip(moves, buffers)):
        reads.append(pltpu.make_async_copy(source, buffer, arrive.at[n]))
        writes.append(pltpu.make_async_copy(buffer, target, leave.at[n]))
    for read in reads:
        read.start()
    for read, write in zip(reads, writes):
        read.wait()
        write.start()
    for write in writes:
        write.wait()


def copy_cost(size):
    return pl.CostEstimate(flops=300 * size, transcendentals=0, bytes_accessed=2 * size)


def block_at(ref, row, row_size, column, column_size):
    return ref.at[pl.ds(pl.multiple_of(row, row_size), row_size), pl.ds(pl.multiple_of(column, column_size), column_size)]


def keep_body(place_ref, old_in, old_out, in_ref, out_ref, in_buffer, out_buffer, arrive, leave, *, kept):
    col = place_ref[2]
    _, tile_rows, tile_cols = old_in.shape
    moves, buffers = [], []
    for j in range(kept):
        target = block_at(in_ref, col * tile_rows, tile_rows, j * tile_cols, tile_cols)
        moves.append((old_in.at[col * kept + j], target))
        buffers.append(in_buffer.at[j])
    for j in range(kept):
        target = block_at(out_ref, j * tile_cols, tile_cols, col * tile_rows, tile_rows)
        moves.append((old_out.at[col * kept + j], target))
        buffers.append(out_buffer.at[j])
    through(moves, buffers, arrive, leave)


def keep_tiles(place, old_in, old_out):
    count, tile_rows, tile_cols = old_in.shape
    kept = count // 2
    hbm = pl.BlockSpec(memory_space=pl.ANY)
    kind = old_in.dtype
    return pl.pallas_call(
        functools.partial(keep_body, kept=kept),
        in_specs=[pl.BlockSpec(memory_space=pltpu.SMEM), hbm, hbm],
        out_specs=[hbm] * 2,
        out_shape=[
            jax.ShapeDtypeStruct((2 * tile_rows, kept * tile_cols), kind),
            jax.ShapeDtypeStruct((kept * tile_cols, 2 * tile_rows), kind),
        ],
        scratch_shapes=[
            pltpu.VMEM((kept, tile_rows, tile_cols), kind),
            pltpu.VMEM((kept, tile_cols, tile_rows), kind),
            pltpu.SemaphoreType.DMA((2 * kept,)),
            pltpu.SemaphoreType.DMA((2 * kept,)),
        ],
        cost_estimate=copy_cost(4 * kept * tile_rows * tile_cols),
        name="keep_tiles",
    )(place, old_in, old_out)


def fill_in_body(place_ref, *refs, parts, counts, rows):
    weight, (buffer, arrive, leave) = refs[-4], refs[-3:]
    rep, row, col = (place_ref[n] for n in range(3))
    moves, buffers, n = [], [], 0
    for k in range(parts):
        first = 0
        for m, count in enumerate(counts):
            part = refs[m * parts + k]
            _, tile_rows, width = part.shape
            for i in range(count):
                column = ((rep ^ k) * rows + (row ^ (first + i))) * width
                target = block_at(weight, (1 - col) * tile_rows, tile_rows, column, width)
                moves.append((part.at[i], target))
                buffers.append(buffer.at[n])
                n += 1
            first += count
    through(moves, buffers, arrive, leave)


def fill(place, parts, weight, body, pieces):
    hbm = pl.BlockSpec(memory_space=pl.ANY)
    return pl.pallas_call(
        body,
        in_specs=[pl.BlockSpec(memory_space=pltpu.SMEM)] + [hbm] * (len(parts) + 1),
        out_specs=hbm,
        out_shape=jax.ShapeDtypeStruct(weight.shape, weight.dtype),
        scratch_shapes=[
            pltpu.VMEM((pieces,) + parts[0].shape[1:], weight.dtype),
            pltpu.SemaphoreType.DMA((pieces,)),
            pltpu.SemaphoreType.DMA((pieces,)),
        ],
        input_output_aliases={1 + len(parts): 0},
        cost_estimate=copy_cost(2 * sum(part.size for part in parts)),
    )(place, *parts, weight)


def cut_body(place_ref, tile_ref, *out_refs):
    row, width = place_ref[1], out_refs[0].shape[-1]
    n = 0
    for ref in out_refs:
        for i in range(ref.shape[0]):
            start = pl.multiple_of((row ^ n) * width, width)
            ref[i] = tile_ref[0, :, pl.ds(start, width)]
            n += 1


def cut_tile(tiles, which, row, counts):
    _, tile_rows, tile_cols = tiles.shape
    width = tile_cols // sum(counts)
    spec = pltpu.PrefetchScalarGridSpec(
        num_scalar_prefetch=1,
        grid=(1,),
        in_specs=[pl.BlockSpec((1, tile_rows, tile_cols), lambda i, s: (s[0], 0, 0))],
        out_specs=[pl.BlockSpec((count, tile_rows, width), lambda i, s: (0, 0, 0)) for count in counts],
    )
    return pl.pallas_call(
        cut_body,
        grid_spec=spec,
        out_shape=[jax.ShapeDtypeStruct((count, tile_rows, width), tiles.dtype) for count in counts],
        name="cut_tile",
    )(jnp.stack([which, row]).astype(jnp.int32), tiles)


def spread(part, axis):
    parts = {0: part}
    for mask in reversed(masks(axis)):
        for k in sorted(parts):
            parts[k ^ mask] = swap(parts[k], axis, mask)
    return [parts[k] for k in sorted(parts)]


CHUNK = 2


def layer_body(place_ref, tokens_ref, scale_ref, bias_ref, tile_ref, *refs, groups, adds):
    pieces = [ref.at[i] for ref in refs[:groups] for i in range(ref.shape[0])]
    sum_ref, hidden_ref, weight = refs[-3:]
    row, width = place_ref[1], pieces[0].shape[-1]

    @pl.when(pl.program_id(0) == 0)
    def _():
        for j, piece in enumerate(pieces):
            weight[:, pl.ds(pl.multiple_of((row ^ j) * width, width), width)] = piece[...]

    tokens, scale = tokens_ref[...], scale_ref[...]
    total = refs[groups][...] if adds else None
    size = weight.shape[1] // CHUNK
    for n in range(CHUNK):
        columns = pl.ds(n * size, size)
        pre = jnp.dot(tokens, weight[:, columns], preferred_element_type=jnp.float32)
        pre = pre * scale + bias_ref[:, columns]
        half = 0.5 * pre
        hidden = (half + half * lax.erf(pre * (0.5**0.5))).astype(jnp.bfloat16)
        hidden_ref[:, columns] = hidden
        term = jnp.dot(hidden, tile_ref[0, columns, :], preferred_element_type=jnp.float32)
        total = term if total is None else total + term
    sum_ref[...] = total.astype(sum_ref.dtype)


def came_body(place_ref, *refs, firsts, shares, halves, fills):
    value_refs, part_refs = refs[:shares], refs[shares : shares * (1 + halves)]
    refs = refs[shares * (1 + halves) + fills :]
    sum_ref, refs = refs[0], refs[1:]
    weight, refs = (refs[0], refs[1:]) if fills else (None, refs)
    values, parts, arrive, leave, total = refs
    rep, col = place_ref[0], place_ref[2]
    count, width = values.shape[1:]
    height, features = parts.shape[1] // halves, parts.shape[2]
    reads = []
    for k in range(shares):
        group = [pltpu.make_async_copy(value_refs[k].at[pl.ds(firsts[k], count)], values.at[k], arrive.at[k, 0])]
        for h in range(halves):
            group.append(
                pltpu.make_async_copy(
                    part_refs[k * halves + h].at[0], parts.at[k, pl.ds(h * height, height)], arrive.at[k, 1 + h]
                )
            )
        for copy in group:
            copy.start()
        reads.append(group)
    writes = []
    for k in range(shares):
        for copy in reads[k]:
            copy.wait()
        if fills:
            target = block_at(weight, (rep ^ k) * width, width, (1 - col) * features, features)
            writes.append(pltpu.make_async_copy(parts.at[k], target, leave.at[k]))
            writes[-1].start()
        term = jnp.dot(values[k], parts[k], preferred_element_type=jnp.float32)
        if k == 0:
            total[...] = term
        elif k < shares - 1:
            total[...] += term
        else:
            sum_ref[...] = (total[...] + term).astype(sum_ref.dtype)
    for copy in writes:
        copy.wait()


def came_sum(place, values, parts, count, kind, weight):
    values, firsts = zip(*values)
    shares, halves = len(values), len(parts) // len(values)
    width, features = values[0].shape[1], parts[0].shape[2]
    hbm = pl.BlockSpec(memory_space=pl.ANY)
    fills = weight is not None
    outs = [jax.ShapeDtypeStruct((count, features), kind)]
    return pl.pallas_call(
        functools.partial(came_body, firsts=firsts, shares=shares, halves=halves, fills=int(fills)),
        in_specs=[pl.BlockSpec(memory_space=pltpu.SMEM)] + [hbm] * (len(values) + len(parts) + fills),
        out_specs=[pl.BlockSpec(memory_space=pltpu.VMEM)] + [hbm] * fills,
        out_shape=outs + ([jax.ShapeDtypeStruct(weight.shape, weight.dtype)] if fills else []),
        scratch_shapes=[
            pltpu.VMEM((shares, count, width), values[0].dtype),
            pltpu.VMEM((shares, width, features), parts[0].dtype),
            pltpu.SemaphoreType.DMA((shares, 1 + halves)),
            pltpu.SemaphoreType.DMA((shares,)),
            pltpu.VMEM((count, features), jnp.float32),
        ],
        input_output_aliases={1 + len(values) + len(parts): 1} if fills else {},
        cost_estimate=pl.CostEstimate(
            flops=2 * count * shares * width * features,
            transcendentals=0,
            bytes_accessed=2 * shares * width * (count + features),
        ),
        name="came_sum",
    )(place, *values, *parts, *((weight,) if fills else ()))


def layer_share(place, tokens, scale, bias, tiles, pieces, total, block, first, count, kind):
    depth = tokens.shape[1]
    _, tile_rows, tile_cols = tiles.shape
    skip = first // block
    same = total is not None and total.shape[0] == count
    spec = pltpu.PrefetchScalarGridSpec(
        num_scalar_prefetch=1,
        grid=(count // block,),
        in_specs=[
            pl.BlockSpec((block, depth), lambda i, s: (i + skip, 0)),
            pl.BlockSpec((block, 1), lambda i, s: (i + skip, 0)),
            pl.BlockSpec(bias.shape, lambda i, s: (0, 0)),
            pl.BlockSpec((1, tile_rows, tile_cols), lambda i, s: (s[0], 0, 0)),
        ]
        + [pl.BlockSpec(piece.shape, lambda i, s: (0, 0, 0)) for piece in pieces]
        + ([] if total is None else [pl.BlockSpec((block, tile_cols), lambda i, s: (i + skip, 0))]),
        out_specs=[
            pl.BlockSpec((block, tile_cols), lambda i, s: (i, 0)),
            pl.BlockSpec((block, tile_rows), lambda i, s: (i, 0)),
        ],
        scratch_shapes=[pltpu.VMEM((depth, tile_rows), tokens.dtype)],
    )
    return pl.pallas_call(
        functools.partial(layer_body, groups=len(pieces), adds=total is not None),
        grid_spec=spec,
        out_shape=[
            jax.ShapeDtypeStruct((count, tile_cols), kind),
            jax.ShapeDtypeStruct((count, tile_rows), jnp.bfloat16),
        ],
        input_output_aliases={5 + len(pieces): 0} if same else {},
        cost_estimate=pl.CostEstimate(
            flops=2 * count * tile_rows * (depth + tile_cols),
            transcendentals=count * tile_rows,
            bytes_accessed=2 * tile_rows * (tile_cols + depth) + count * (8 * tile_cols + 2 * tile_rows),
        ),
        name="layer_share",
    )(place, tokens, scale, bias, tiles, *pieces, *(() if total is None else (total,)))


def move_halves(pieces, axis):
    index = lax.axis_index(axis)
    for bit, mask in enumerate(masks(axis)):
        upper_side = index >> bit & 1 == 1
        outgoing = tuple(jnp.where(upper_side, low, high) for low, high in pieces)
        incoming = tuple(swap(part, axis, mask) for part in outgoing)
        pieces = tuple(
            (jnp.where(upper_side, came, low), jnp.where(upper_side, high, came))
            for (low, high), came in zip(pieces, incoming)
        )
    return pieces


def relayout_any(old_in, old_out):
    tiles_here, tile_rows, tile_cols = old_in.shape
    local_cols = tiles_here * tile_cols
    half = local_cols // 2
    in_local = jnp.transpose(old_in, (1, 0, 2)).reshape(tile_rows, local_cols)
    out_local = old_out.reshape(local_cols, tile_rows)
    in_pair, out_pair = move_halves(
        ((in_local[:, :half], in_local[:, half:]), (out_local[:half], out_local[half:])), "col"
    )
    return jnp.concatenate(in_pair, axis=0), jnp.concatenate(out_pair, axis=1)


def on_device(
    patches,
    embed_weight,
    embed_bias,
    old_in,
    old_out,
    restore_id,
    norm_gains,
    in_biases,
    out_biases,
    final_gain,
    check_weight,
):
    reps, rows, cols = (lax.axis_size(axis) for axis in ("rep", "row", "col"))
    rep, row, col = (lax.axis_index(axis) for axis in ("rep", "row", "col"))
    tiles_here, tile_rows, tile_cols = old_in.shape
    tokens, patch = patches.shape
    features = embed_weight.shape[1]
    feature_count = features * rows
    depth = -(-(patch + 1) // 16) * 16
    pair = cols == 2 and reps == 4 and tiles_here == 2 * reps and features == 2 * tile_rows and tile_cols % (128 * rows) == 0

    if pair:
        kept = tiles_here // 2
        own, away = col * kept, (1 - col) * kept
        cut = [rows // 2, rows - rows // 2]
        in_sent = cut_tile(old_in, away + rep, row, cut)
        in_sent, embed_weight, embed_bias, patches = lax.optimization_barrier(
            (in_sent, embed_weight, embed_bias, patches)
        )
        in_came = [None] * len(cut)
        for m in reversed(range(len(cut))):
            in_came[m] = swap(in_sent[m], "col", 1)
        in_mine = cut_tile(old_in, own + rep, row, cut)
        where = jnp.stack([rep, row, col]).astype(jnp.int32)
        in_weight, out_weight = keep_tiles(where, old_in, old_out)
    else:
        in_weight, out_weight = relayout_any(old_in, old_out)

    def mine_first(values, axis):
        return jnp.roll(values, -col * tile_rows, axis) if pair else values

    layer_gain = mine_first(row_of(norm_gains, restore_id), 0)
    in_bias = row_of(in_biases, restore_id)
    out_bias = mine_first(row_of(out_biases, restore_id), 0)
    embed_weight = mine_first(embed_weight, 1)
    embed_bias = mine_first(embed_bias, 0)
    final_gain = mine_first(final_gain, 0)
    check_weight = mine_first(check_weight, 0)

    embedded = jnp.dot(patches, embed_weight, preferred_element_type=jnp.float32) + embed_bias
    weight_f32 = embed_weight.astype(jnp.float32)
    sums = all_sum(
        jnp.concatenate(
            [
                jnp.sum(embedded, axis=1),
                jnp.sum(embedded * embedded, axis=1),
                jnp.sum(weight_f32, axis=1),
                jnp.sum(embed_bias)[None],
            ]
        ),
        "row",
    ) / feature_count
    average, square = sums[:tokens], sums[tokens : 2 * tokens]
    scale = gather_xor(lax.rsqrt(square - average * average + EPSILON), "col")[:, None]

    centers = sums[2 * tokens :]
    centered = jnp.concatenate(
        [
            (weight_f32 - centers[:patch, None]) * layer_gain,
            ((embed_bias - centers[patch]) * layer_gain)[None],
            jnp.zeros((depth - patch - 1, features), jnp.float32),
        ]
    ).astype(jnp.bfloat16)
    hidden_here = in_weight.shape[1]
    share = hidden_here // reps
    piece = share // rows

    def times(left, right):
        return jnp.dot(left, right, preferred_element_type=jnp.float32)

    def partial(k):
        if not pair:
            return times(centered, lax.dynamic_slice_in_dim(in_weight, rep * share + (row ^ k) * piece, piece, 1))
        m, i = (0, k) if k < cut[0] else (1, k - cut[0])
        return times(centered[:, :tile_rows], in_mine[m][i]) + times(centered[:, tile_rows:], in_came[m][i])

    first_sent = partial(rows - 1).astype(jnp.bfloat16)
    one, late, first_sent = lax.optimization_barrier((jnp.ones((tokens, 1), patches.dtype), (1 - col) * (tiles_here // 2), first_sent))
    tokens_in = jnp.concatenate(
        [patches, one, jnp.zeros((tokens, depth - patch - 1), patches.dtype)], axis=1
    )
    tokens_in = gather_xor(tokens_in, "col")
    if pair:
        height = tile_cols // 2

        def out_half(k, half):
            sent = lax.dynamic_slice(old_out, (late + (rep ^ k), half * height, 0), (1, height, tile_rows))
            return swap(sent, "col", 1)

        out_parts = {(0, 0): out_half(0, 0), (0, 1): out_half(0, 1), (2, 1): out_half(2, 1)}

    came = [swap(first_sent, "row", rows - 1)]
    came += [swap(partial(k).astype(jnp.bfloat16), "row", k) for k in reversed(range(1, rows - 1))]
    folded = partial(0)
    for value in came:
        folded = folded + value.astype(jnp.float32)
    folded = folded.astype(jnp.bfloat16)
    group = spread(folded, "row")

    if pair:
        groups = {0: group}
        for mask in reversed(masks("rep")):
            for k in sorted(groups):
                if mask > 1:
                    groups[k ^ mask] = [swap(value, "rep", mask) for value in groups[k]]
                else:
                    joined = jnp.stack(groups[k])
                    groups[k ^ mask] = [swap(joined, "rep", mask)]
        in_parts = [spread(part, "rep") for part in in_came]
        out_parts[2, 0] = swap(out_parts[0, 0], "rep", 2)
        for k, half in sorted(out_parts):
            out_parts[k ^ 1, half] = swap(out_parts[k, half], "rep", 1)
        in_weight = fill(
            where,
            [part for parts in in_parts for part in parts],
            in_weight,
            functools.partial(fill_in_body, parts=reps, counts=cut, rows=rows),
            reps * rows,
        )
        biases = in_bias.reshape(reps, 1, share)
        order = sorted(groups, key=lambda k: (bin(k).count("1"), k))
        block = min(256, tokens)

        def layer(k, total, first, count, kind):
            pieces = [value if value.ndim == 3 else value[None] for value in groups[k]]
            place = jnp.stack([own + (rep ^ k), row]).astype(jnp.int32)
            bias = lax.dynamic_index_in_dim(biases, rep ^ k, 0, keepdims=False)
            return layer_share(place, tokens_in, scale, bias, old_out, pieces, total, block, first, count, kind)

        branch_mine, values = None, {}
        for k in order[:-1]:
            branch_mine, values[k] = layer(k, branch_mine, 0, 2 * tokens, jnp.float32)
        last = order[-1]
        theirs, value_theirs = layer(last, branch_mine, tokens, tokens, jnp.bfloat16)
        to_came = swap(theirs, "col", 1).astype(jnp.float32)
        branch_mine, value_ours = layer(last, branch_mine, 0, tokens, jnp.float32)
        parts = [out_parts[key] for key in sorted(out_parts)]
        shares = [(values[k], tokens) for k in sorted(values)] + [(value_theirs, 0)]
        theirs, out_weight = came_sum(where, shares, parts, tokens, jnp.bfloat16, out_weight)
        to_mine = swap(theirs, "col", 1).astype(jnp.float32)
        shares = [(values[k], 0) for k in sorted(values)] + [(value_ours, 0)]
        (branch_came,) = came_sum(where, shares, parts, tokens, jnp.float32, None)
        branch = jnp.concatenate([branch_mine + to_mine, branch_came + to_came], axis=1)
    else:
        group = jnp.take(jnp.stack(group), row ^ jnp.arange(rows), axis=0)
        shares = jnp.take(jnp.stack(spread(group, "rep")), rep ^ jnp.arange(reps), axis=0)
        folded = jnp.transpose(shares, (2, 0, 1, 3)).reshape(depth, hidden_here)
        pre = times(tokens_in, folded) * scale + in_bias
        hidden = (0.5 * pre * (1.0 + lax.erf(pre * (0.5**0.5)))).astype(jnp.bfloat16)
        branch = scatter_xor(times(hidden, out_weight), "col")
    updated = embedded + branch + out_bias

    center = jnp.mean(updated, axis=1, keepdims=True)
    weighted = final_gain[:, None] * check_weight.astype(jnp.float32)
    slope = jnp.sum(weighted, axis=0, keepdims=True)
    logits = times(((updated - center) * final_gain).astype(jnp.bfloat16), check_weight) + center * slope
    checks = logits.shape[1]
    moments = jnp.concatenate([jnp.sum(updated, axis=1), jnp.sum(updated * updated, axis=1), slope[0]])
    moments = jnp.pad(moments, (0, -moments.size % (8 * checks))).reshape(-1, checks)
    total = all_sum(jnp.concatenate([logits, moments]), "row")
    moments = total[tokens:].reshape(-1)
    average = moments[:tokens, None] / feature_count
    variance = moments[tokens : 2 * tokens, None] / feature_count - average * average
    slope = moments[None, 2 * tokens : 2 * tokens + checks]
    check_logits = (total[:tokens] - average * slope) * lax.rsqrt(variance + EPSILON)
    return (in_weight, out_weight, check_logits)


def solution(mesh):
    placed = (
        P(("rep", "col"), None),
        P(None, "row"),
        P("row"),
        P(("row", "col"), None, None),
        P(("row", "col"), None, None),
        P(),
        P(None, "row"),
        P(None, "col"),
        P(None, "row"),
        P("row"),
        P("row", None),
    )
    return jax.shard_map(
        on_device,
        mesh=mesh,
        in_specs=placed,
        out_specs=(P("row", "col"), P("col", "row"), P(("rep", "col"), None)),
        check_vma=False,
    )
```
